32 devices in a mesh: row: 4 (over y, x), col: 4 (over z), fiber: 2 (over core).
Axes of the slice: x: 2, y: 2, z: 4, core: 2. Of those that a mesh axis runs over, the one named last changes fastest.
Arguments:
- user_factors: float32 [8192, 128], P(('row', 'col', 'fiber')), may hold values from -3 to 3
- item_factors: bfloat16 [16384, 128], P(('row', 'col')), may hold values from -0.119628906 to 0.119628906
- ratings: bfloat16 [4, 4, 256, 128, 128], P('row', 'col', 'fiber'), may hold values from -2 to 2, as said below
- block_user: int32 [4, 4, 256], P('row', 'col', 'fiber'), may hold values from 0 to 15, as said below
- block_item: int32 [4, 4, 256], P('row', 'col', 'fiber'), may hold values from 0 to 31, as said below
- counts: int32 [8192], P(('row', 'col', 'fiber')), may hold values from 1 to 8192, as said below
Outputs:
- factors: float32 [8192, 128], P(('row', 'col', 'fiber'))
- residual: float32 [8192, 128], P(('row', 'col', 'fiber'))
The draws below stay inside these ranges and needn't reach their ends.
Inputs may be any that keep to these rules, and one draw needn't show every extreme that they name: `block_user`: within one tile (one row index and one column index) the occupied blocks are distinct; each user block index appears in exactly 16 blocks of every tile, which fall on the two fiber halves at random. `block_item`: an item block index within the column slab. counts[u] equals the number of nonzero entries of ratings that belong to user u, over all blocks; some user has every rating of its blocks observed. Every user row of every occupied block has an observed rating; observed ratings have magnitude 0.25 or more.
All inputs are finite; a program needn't handle non-finite values.
Results may differ from the reference program's by a relative error of at most 0.012.
The reference program's roundings to bfloat16 on the way count: a program that leaves them out, or rounds other values in their place, can miss the bound.
Values may be sent and summed in bfloat16 or wider, within the bound.
A program may use at most 64 MiB of HBM per device.

```python
import jax
import jax.numpy as jnp
from jax import lax

RANK = 128
BLOCK = 128
ITERS = 2
ITEM_DEV = 1024
GRID_ROWS = 4
GRID_COLS = 4
TILE_BLOCKS = 256
USER_BLOCKS = 16
ITEM_BLOCKS = 32
BLOCKS_PER_USER = 16
USERS = 8192
ITEMS = 16384


def layout(key):
    base = jax.random.fold_in(key, 7001)
    tiles = GRID_ROWS * GRID_COLS
    perm_keys = jax.random.split(jax.random.fold_in(base, 1), tiles * USER_BLOCKS)
    perms = jax.vmap(lambda sub: jax.random.permutation(sub, ITEM_BLOCKS))(perm_keys)
    chosen = perms[:, :BLOCKS_PER_USER].reshape(tiles, TILE_BLOCKS).astype(jnp.int32)
    owners = jnp.repeat(jnp.arange(USER_BLOCKS, dtype=jnp.int32), BLOCKS_PER_USER)
    owners = jnp.broadcast_to(owners[None, :], (tiles, TILE_BLOCKS))
    order_keys = jax.random.split(jax.random.fold_in(base, 2), tiles)
    orders = jax.vmap(lambda sub: jax.random.permutation(sub, TILE_BLOCKS))(order_keys)
    users = jnp.take_along_axis(owners, orders, axis=1)
    items = jnp.take_along_axis(chosen, orders, axis=1)
    return (users.reshape(GRID_ROWS, GRID_COLS, TILE_BLOCKS), items.reshape(GRID_ROWS, GRID_COLS, TILE_BLOCKS))


def observed_entries(key):
    users, items = layout(key)
    base = jax.random.fold_in(key, 7002)
    density = jax.random.randint(jax.random.fold_in(base, 1), (USERS,), 1, 9)
    dense_user = jax.random.randint(jax.random.fold_in(base, 4), (), 0, USERS)
    density = jnp.where(jnp.arange(USERS, dtype=jnp.int32) == dense_user, 16, density)
    grid_rows = jnp.arange(GRID_ROWS, dtype=jnp.int32)[:, None, None, None]
    inside = jnp.arange(BLOCK, dtype=jnp.int32)[None, None, None, :]
    user_ids = grid_rows * (USER_BLOCKS * BLOCK) + users[..., None] * BLOCK + inside
    levels = density[user_ids]
    random_bits = jax.random.randint(jax.random.fold_in(base, 2), (GRID_ROWS, GRID_COLS, TILE_BLOCKS, BLOCK, BLOCK), 0, 16)
    forced = jax.random.randint(jax.random.fold_in(base, 3), (GRID_ROWS, GRID_COLS, TILE_BLOCKS, BLOCK), 0, BLOCK)
    column_ids = jnp.arange(BLOCK, dtype=jnp.int32)
    chosen = (random_bits < levels[..., None]) | (column_ids == forced[..., None])
    return (chosen, user_ids)


def draw_block_user(key, part):
    return layout(key)[0]


def draw_block_item(key, part):
    return layout(key)[1]


def draw_counts(key, part):
    chosen, user_ids = observed_entries(key)
    per_row = jnp.sum(chosen.astype(jnp.int32), axis=-1)
    totals = jnp.zeros((USERS,), jnp.int32)
    return totals.at[user_ids.reshape(-1)].add(per_row.reshape(-1))


def draw_ratings(key, part):
    chosen, user_ids = observed_entries(key)
    base = jax.random.fold_in(key, 7003)
    shape = (GRID_ROWS, GRID_COLS, TILE_BLOCKS, BLOCK, BLOCK)
    uniform = jax.random.uniform(jax.random.fold_in(base, 1), shape, jnp.float32)
    coins = jax.random.uniform(jax.random.fold_in(base, 2), shape, jnp.float32)
    signs = jnp.where(coins < 0.5, 1.0, -1.0)
    magnitude = 0.25 + 1.75 * uniform
    values = jnp.where(chosen, signs * magnitude, 0.0)
    return values.astype(jnp.bfloat16)


def block_scale(own_key, shape, cuts, least, top_value):
    factor_of = 1.0
    for position, shards_of in cuts:
        draws = jax.random.uniform(jax.random.fold_in(jax.random.fold_in(own_key, 6), position), (shards_of,), jnp.float32, least / len(cuts), top_value / len(cuts))
        factor_of = factor_of * jnp.repeat(jnp.exp(draws), shape[position] // shards_of).reshape((-1,) + (1,) * (len(shape) - 1 - position))
    return factor_of


def scatter_about(key, dims, spread, bound, shards=(), kind=jnp.bfloat16):
    array = spread * jax.random.normal(key, dims, jnp.float32)
    if shards:
        array = array * block_scale(key, dims, shards, -0.22, 0.18)
    return jnp.clip(array, -bound, bound).astype(kind)


def setup_inputs(seed: int = 0) -> dict:
    key_of = jax.random.split(jax.random.key(seed), 7)
    user_factors = scatter_about(key_of[0], (USERS, RANK), 0.5, 3.0, ((0, 32),), jnp.float32)
    item_factors = scatter_about(key_of[1], (ITEMS, RANK), 0.02, 0.119628906, ((0, 16),))
    ratings = draw_ratings(jax.random.fold_in(key_of[6], 71), 0)
    block_user = draw_block_user(jax.random.fold_in(key_of[6], 71), 0)
    block_item = draw_block_item(jax.random.fold_in(key_of[6], 71), 0)
    counts = draw_counts(jax.random.fold_in(key_of[6], 71), 0)
    return {"user_factors": user_factors, "item_factors": item_factors, "ratings": ratings, "block_user": block_user, "block_item": block_item, "counts": counts}


reg_weight = 4e-4
tiny = 1e-6


def block_terms(slab_values, item_slab, rating_tile, owners, columns, with_ratings):
    block_size = rating_tile.shape[1]
    factor_rank = slab_values.shape[1]
    user_count = slab_values.shape[0] // block_size
    user_rows = slab_values.reshape(user_count, block_size, factor_rank)[owners].astype(jnp.float32)
    item_rows = item_slab.reshape(item_slab.shape[0] // block_size, block_size, factor_rank)[columns].astype(jnp.float32)
    predicted = jnp.einsum("nik,njk->nij", user_rows, item_rows)
    observed = (rating_tile != 0).astype(jnp.float32)
    if with_ratings:
        weights = (rating_tile.astype(jnp.float32) - observed * predicted).astype(jnp.bfloat16)
    else:
        weights = (observed * predicted).astype(jnp.bfloat16)
    weights = lax.optimization_barrier(weights).astype(jnp.float32)
    contribution = jnp.einsum("nij,njk->nik", weights, item_rows)
    summed = jax.ops.segment_sum(contribution, owners, num_segments=user_count)
    return summed.reshape(user_count * block_size, factor_rank)


def apply_all(values, item_factors, ratings, block_user, block_item, with_ratings):
    user_grid = values.reshape(GRID_ROWS, USER_BLOCKS * BLOCK, RANK)
    item_grid = item_factors.reshape(GRID_ROWS, GRID_COLS, ITEM_DEV, RANK)
    col_index = jnp.arange(GRID_COLS, dtype=jnp.int32)

    def per_row(grid_row):
        def per_col(running, grid_col):
            item_slab = item_grid[:, grid_col].reshape(GRID_ROWS * ITEM_DEV, RANK)
            term = block_terms(user_grid[grid_row], item_slab, ratings[grid_row, grid_col], block_user[grid_row, grid_col], block_item[grid_row, grid_col], with_ratings)
            return running + term, None

        initial = jnp.zeros((USER_BLOCKS * BLOCK, RANK), jnp.float32)
        running, unused = lax.scan(per_col, initial, col_index)
        return running

    stacked = lax.map(per_row, jnp.arange(GRID_ROWS, dtype=jnp.int32))
    return stacked.reshape(USERS, RANK)


def reference(user_factors, item_factors, ratings, block_user, block_item, counts):
    damping = reg_weight * counts.astype(jnp.float32)[:, None]
    factors = user_factors
    residual = apply_all(factors.astype(jnp.bfloat16), item_factors, ratings, block_user, block_item, True) - damping * factors
    direction = residual
    squares = jnp.sum(residual * residual, axis=1, keepdims=True)
    for iteration in range(ITERS):
        image = apply_all(direction.astype(jnp.bfloat16), item_factors, ratings, block_user, block_item, False) + damping * direction
        step_size = squares / (jnp.sum(direction * image, axis=1, keepdims=True) + tiny)
        factors = factors + step_size * direction
        residual = residual - step_size * image
        if iteration + 1 < ITERS:
            renewed = jnp.sum(residual * residual, axis=1, keepdims=True)
            direction = residual + (renewed / (squares + tiny)) * direction
            squares = renewed
    return factors, residual
```

```python
import functools

import jax
import jax.numpy as jnp
from jax import lax
from jax.experimental import pallas as pl
from jax.experimental.pallas import tpu as pltpu
from jax.sharding import PartitionSpec as P

ITERS = 2
GROUP = 4

reg_weight = 0.0004
tiny = 1e-06

MESH = pl.DeviceIdType.MESH


def sweep_kernel(
    sizes, pos_ref, item_ref, uf_ref, damp_ref, items_hbm, ratings_hbm, x_ref, r_ref,
    vbuf, rbuf, pbuf, part, recv, p_ref,
    item_sem, rating_sem, v_send, v_recv, d_send, d_recv, t_send, t_recv, g_send, g_recv, s_send, s_recv,
):
    rows, cols, fibers = sizes
    my_row, my_col, my_fiber = lax.axis_index("row"), lax.axis_index("col"), lax.axis_index("fiber")
    held_items = items_hbm.shape[0]
    share = held_items // fibers
    held_blocks, block = ratings_hbm.shape[0], ratings_hbm.shape[1]
    own_users = uf_ref.shape[0] // block
    per_user = pos_ref.shape[0] // (cols * own_users)

    def row_of(d):
        return lax.rem(my_row + d, rows)

    def col_of(d):
        return lax.rem(my_col + d, cols)

    def fiber_of(d):
        return lax.rem(my_fiber + d, fibers)

    own_items = pl.ds(my_row * held_items, held_items)
    item_load = pltpu.make_async_copy(items_hbm, vbuf.at[own_items], item_sem)
    item_load.start()
    own_ratings = pl.ds(my_fiber * held_blocks, held_blocks)
    rating_load = pltpu.make_async_copy(ratings_hbm, rbuf.at[own_ratings], rating_sem)
    rating_load.start()

    barrier = pltpu.get_barrier_semaphore()
    for d in range(1, rows):
        pl.semaphore_signal(barrier, inc=1, device_id={"row": row_of(d)}, device_id_type=MESH)
    for d in range(1, cols):
        pl.semaphore_signal(barrier, inc=1, device_id={"col": col_of(d)}, device_id_type=MESH)
    for d in range(1, fibers):
        pl.semaphore_signal(barrier, inc=1, device_id={"fiber": fiber_of(d)}, device_id_type=MESH)

    pbuf[0, my_col] = uf_ref[...].astype(jnp.bfloat16)
    pl.semaphore_wait(barrier, rows + cols + fibers - 3)

    def gather_copy(stage, d):
        return pltpu.make_async_remote_copy(
            src_ref=pbuf.at[stage, my_col],
            dst_ref=pbuf.at[stage, my_col],
            send_sem=g_send.at[stage, d],
            recv_sem=g_recv.at[stage, d],
            device_id={"col": col_of(d)},
            device_id_type=MESH,
        )

    def scatter_copy(stage, d):
        return pltpu.make_async_remote_copy(
            src_ref=part.at[stage, d],
            dst_ref=recv.at[stage, d],
            send_sem=s_send.at[stage, d],
            recv_sem=s_recv.at[stage, d],
            device_id={"col": col_of(d)},
            device_id_type=MESH,
        )

    item_sends = []
    for d in range(1, rows):
        copy = pltpu.make_async_remote_copy(
            src_ref=items_hbm.at[pl.ds(my_fiber * share, share)],
            dst_ref=vbuf.at[pl.ds(my_row * held_items + my_fiber * share, share)],
            send_sem=v_send.at[d],
            recv_sem=v_recv.at[d],
            device_id={"row": row_of(d)},
            device_id_type=MESH,
        )
        copy.start()
        item_sends.append(copy)
    for d in range(1, cols):
        gather_copy(0, d).start()
    rating_sends = []
    for e in range(1, fibers):
        copy = pltpu.make_async_remote_copy(
            src_ref=ratings_hbm,
            dst_ref=rbuf.at[own_ratings],
            send_sem=t_send.at[e],
            recv_sem=t_recv.at[e],
            device_id={"fiber": fiber_of(e)},
            device_id_type=MESH,
        )
        copy.start()
        rating_sends.append(copy)
    shared = []
    for d in range(1, rows):
        item_sends[d - 1].wait_recv()
        source = lax.rem(my_row + rows - d, rows)
        piece = pl.ds(source * held_items + my_fiber * share, share)
        for e in range(1, fibers):
            copy = pltpu.make_async_remote_copy(
                src_ref=vbuf.at[piece],
                dst_ref=vbuf.at[piece],
                send_sem=d_send.at[d, e],
                recv_sem=d_recv.at[d, e],
                device_id={"fiber": fiber_of(e)},
                device_id_type=MESH,
            )
            copy.start()
            shared.append(copy)
    item_load.wait()
    rating_load.wait()
    for copy in rating_sends + shared:
        copy.wait_recv()

    def user_terms(stage, col, j):
        rows_of_user = pbuf[stage, col, pl.ds(pl.multiple_of(j * block, block), block), :]
        base = (col * own_users + j) * per_user

        def visit(g, total):
            first = base + g * GROUP
            items = jnp.concatenate([vbuf[item_ref[first + i]] for i in range(GROUP)], axis=0)
            ratings = jnp.concatenate([rbuf[pos_ref[first + i]] for i in range(GROUP)], axis=1)
            predicted = lax.dot_general(
                rows_of_user, items, (((1,), (1,)), ((), ())), preferred_element_type=jnp.float32
            )
            ratings = ratings.astype(jnp.float32)
            if stage == 0:
                weights = jnp.where(ratings != 0, ratings - predicted, 0.0)
            else:
                weights = jnp.where(ratings != 0, predicted, 0.0)
            return total + jnp.dot(
                weights.astype(jnp.bfloat16), items, preferred_element_type=jnp.float32
            )

        return lax.fori_loop(0, per_user // GROUP, visit, jnp.zeros((block, items_hbm.shape[2]), jnp.float32))

    def reduced(stage):
        for d in list(range(1, cols)) + [0]:
            if d:
                pltpu.make_async_remote_copy(
                    src_ref=pbuf.at[stage, my_col],
                    dst_ref=pbuf.at[stage, my_col],
                    send_sem=g_send.at[stage, cols - d],
                    recv_sem=g_recv.at[stage, cols - d],
                    device_id={"col": col_of(cols - d)},
                    device_id_type=MESH,
                ).wait_recv()
            col = col_of(d)

            def one(j, carry):
                part[stage, d, pl.ds(pl.multiple_of(j * block, block), block), :] = user_terms(stage, col, j)
                return carry

            lax.fori_loop(0, own_users, one, 0)
            if d:
                scatter_copy(stage, d).start()
        total = part[stage, 0]
        for d in range(1, cols):
            scatter_copy(stage, d).wait_recv()
            total = total + recv[stage, d]
        return total

    x_ref[...] = uf_ref[...]
    residual = reduced(0) - damp_ref[...] * uf_ref[...]
    r_ref[...] = residual
    p_ref[...] = residual
    squares = jnp.sum(residual * residual, axis=1, keepdims=True)
    for iteration in range(ITERS):
        pbuf[iteration + 1, my_col] = p_ref[...].astype(jnp.bfloat16)
        for d in range(1, cols):
            gather_copy(iteration + 1, d).start()
        image = reduced(iteration + 1) + damp_ref[...] * p_ref[...]
        direction = p_ref[...]
        step_size = squares / (jnp.sum(direction * image, axis=1, keepdims=True) + tiny)
        x_ref[...] = x_ref[...] + step_size * direction
        residual = r_ref[...] - step_size * image
        r_ref[...] = residual
        if iteration + 1 < ITERS:
            renewed = jnp.sum(residual * residual, axis=1, keepdims=True)
            p_ref[...] = residual + renewed / (squares + tiny) * direction
            squares = renewed

    for copy in item_sends + rating_sends + shared:
        copy.wait_send()
    for stage in range(ITERS + 1):
        for d in range(1, cols):
            gather_copy(stage, d).wait_send()
            scatter_copy(stage, d).wait_send()


def per_device(sizes, slab_users, user_factors, item_factors, ratings, block_user, block_item, counts):
    rows, cols, fibers = sizes
    held_blocks, block = ratings.shape[2], ratings.shape[3]
    rank = user_factors.shape[1]
    users = user_factors.shape[0]
    own_users = users // block
    item_blocks = item_factors.shape[0] // block
    per_user = fibers * held_blocks // (slab_users // block)

    both = lax.all_gather(jnp.stack([block_user[0, 0], block_item[0, 0]]), "fiber", axis=0)
    owners = both[:, 0].reshape(-1)
    columns = both[:, 1].reshape(-1)
    here = jnp.arange(owners.shape[0], dtype=jnp.int32)
    keys = owners * owners.shape[0] + here
    ranks = jnp.sum((keys[None, :] < keys[:, None]).astype(jnp.int32), axis=1)
    groups = jnp.arange(cols, dtype=jnp.int32)[:, None] * fibers + lax.axis_index("fiber")
    wanted = (
        groups[:, :, None] * (own_users * per_user)
        + jnp.arange(own_users * per_user, dtype=jnp.int32)[None, None, :]
    ).reshape(-1)
    match = wanted[:, None] == ranks[None, :]
    positions = jnp.sum(jnp.where(match, here[None, :], 0), axis=1)
    items = jnp.sum(jnp.where(match, columns[None, :], 0), axis=1)
    damping = jnp.broadcast_to(reg_weight * counts.astype(jnp.float32)[:, None], (users, rank))

    stages = ITERS + 1
    dma = pltpu.SemaphoreType.DMA
    vmem = pl.BlockSpec(memory_space=pltpu.VMEM)
    smem = pl.BlockSpec(memory_space=pltpu.SMEM)
    hbm = pl.BlockSpec(memory_space=pl.ANY)
    return pl.pallas_call(
        functools.partial(sweep_kernel, sizes),
        out_shape=(
            jax.ShapeDtypeStruct((users, rank), jnp.float32),
            jax.ShapeDtypeStruct((users, rank), jnp.float32),
        ),
        in_specs=[smem, smem, vmem, vmem, hbm, hbm],
        out_specs=(vmem, vmem),
        scratch_shapes=[
            pltpu.VMEM((rows * item_blocks, block, rank), jnp.bfloat16),
            pltpu.VMEM((fibers * held_blocks, block, block), jnp.bfloat16),
            pltpu.VMEM((stages, cols, users, rank), jnp.bfloat16),
            pltpu.VMEM((stages, cols, users, rank), jnp.float32),
            pltpu.VMEM((stages, cols, users, rank), jnp.float32),
            pltpu.VMEM((users, rank), jnp.float32),
            dma,
            dma,
            dma((rows,)),
            dma((rows,)),
            dma((rows, fibers)),
            dma((rows, fibers)),
            dma((fibers,)),
            dma((fibers,)),
            dma((stages, cols)),
            dma((stages, cols)),
            dma((stages, cols)),
            dma((stages, cols)),
        ],
        compiler_params=pltpu.CompilerParams(
            collective_id=0, has_side_effects=True, vmem_limit_bytes=48 * 1024 * 1024
        ),
    )(
        positions,
        items,
        user_factors,
        damping,
        item_factors.reshape(item_blocks, block, rank),
        ratings[0, 0],
    )


def solution(mesh):
    sizes = (mesh.shape["row"], mesh.shape["col"], mesh.shape["fiber"])

    def whole(user_factors, item_factors, ratings, block_user, block_item, counts):
        slab_users = user_factors.shape[0] // sizes[0]
        return jax.shard_map(
            functools.partial(per_device, sizes, slab_users),
            mesh=mesh,
            in_specs=(
                P(("row", "col", "fiber"), None),
                P(("row", "col"), None),
                P("row", "col", "fiber", None, None),
                P("row", "col", "fiber"),
                P("row", "col", "fiber"),
                P(("row", "col", "fiber")),
            ),
            out_specs=(P(("row", "col", "fiber"), None), P(("row", "col", "fiber"), None)),
            check_vma=False,
        )(user_factors, item_factors, ratings, block_user, block_item, counts)

    return whole
```

```python
import functools

import jax
import jax.numpy as jnp
from jax import lax
from jax.experimental import pallas as pl
from jax.experimental.pallas import tpu as pltpu
from jax.sharding import PartitionSpec as P

ITERS = 2

reg_weight = 0.0004
tiny = 1e-06

MESH = pl.DeviceIdType.MESH


def sweep_kernel(
    sizes, pos_ref, item_ref, uf_hbm, counts_hbm, items_hbm, ratings_hbm, x_ref, r_ref,
    vbuf, rbuf, pbuf, part, recv, p_ref, damp_ref, counts_ref,
    user_sem, count_sem, item_sem, rating_sem, v_send, v_recv, d_send, d_recv, t_send, t_recv, g_send, g_recv, s_send, s_recv,
):
    rows, cols, fibers = sizes
    my_row, my_col, my_fiber = lax.axis_index("row"), lax.axis_index("col"), lax.axis_index("fiber")
    held_items = items_hbm.shape[0]
    share = held_items // fibers
    held_blocks, block = ratings_hbm.shape[0], ratings_hbm.shape[1]
    own_users = uf_hbm.shape[0] // block
    per_user = pos_ref.shape[0] // (cols * own_users)

    def row_of(d):
        return lax.rem(my_row + d, rows)

    def col_of(d):
        col, bit = my_col, 1
        while bit <= d:
            if d & bit:
                col = col + bit * (1 - 2 * lax.rem(lax.div(my_col, bit), 2))
            bit *= 2
        return col

    def fiber_of(d):
        return lax.rem(my_fiber + d, fibers)

    user_load = pltpu.make_async_copy(uf_hbm, x_ref, user_sem)
    user_load.start()
    count_load = pltpu.make_async_copy(counts_hbm, counts_ref, count_sem)
    count_load.start()
    own_items = pl.ds(my_row * held_items, held_items)
    item_load = pltpu.make_async_copy(items_hbm, vbuf.at[own_items], item_sem)
    item_load.start()
    own_ratings = pl.ds(my_fiber * held_blocks, held_blocks)
    rating_load = pltpu.make_async_copy(ratings_hbm, rbuf.at[own_ratings], rating_sem)
    rating_load.start()

    barrier = pltpu.get_barrier_semaphore()
    for d in range(1, rows):
        pl.semaphore_signal(barrier, inc=1, device_id={"row": row_of(d)}, device_id_type=MESH)
    for d in range(1, cols):
        pl.semaphore_signal(barrier, inc=1, device_id={"col": col_of(d)}, device_id_type=MESH)
    for d in range(1, fibers):
        pl.semaphore_signal(barrier, inc=1, device_id={"fiber": fiber_of(d)}, device_id_type=MESH)

    user_load.wait()
    pbuf[0, my_col] = x_ref[...].astype(jnp.bfloat16)
    pl.semaphore_wait(barrier, rows + cols + fibers - 3)

    def gather_copy(stage, d):
        return pltpu.make_async_remote_copy(
            src_ref=pbuf.at[stage, my_col],
            dst_ref=pbuf.at[stage, my_col],
            send_sem=g_send.at[stage, d],
            recv_sem=g_recv.at[stage, d],
            device_id={"col": col_of(d)},
            device_id_type=MESH,
        )

    def scatter_copy(stage, d, j):
        return pltpu.make_async_remote_copy(
            src_ref=part.at[stage, d, j],
            dst_ref=recv.at[stage, d, j],
            send_sem=s_send.at[stage, d, j],
            recv_sem=s_recv.at[stage, d, j],
            device_id={"col": col_of(d & -d)},
            device_id_type=MESH,
        )

    item_sends = []
    for d in range(1, rows):
        copy = pltpu.make_async_remote_copy(
            src_ref=items_hbm.at[pl.ds(my_fiber * share, share)],
            dst_ref=vbuf.at[pl.ds(my_row * held_items + my_fiber * share, share)],
            send_sem=v_send.at[d],
            recv_sem=v_recv.at[d],
            device_id={"row": row_of(d)},
            device_id_type=MESH,
        )
        copy.start()
        item_sends.append(copy)
    order = sorted(range(1, cols), key=lambda d: (d & -d, -d))
    for d in order:
        gather_copy(0, d).start()
    rating_sends = []
    for e in range(1, fibers):
        copy = pltpu.make_async_remote_copy(
            src_ref=ratings_hbm,
            dst_ref=rbuf.at[own_ratings],
            send_sem=t_send.at[e],
            recv_sem=t_recv.at[e],
            device_id={"fiber": fiber_of(e)},
            device_id_type=MESH,
        )
        copy.start()
        rating_sends.append(copy)
    shared = []
    for d in range(1, rows):
        item_sends[d - 1].wait_recv()
        source = lax.rem(my_row + rows - d, rows)
        piece = pl.ds(source * held_items + my_fiber * share, share)
        for e in range(1, fibers):
            copy = pltpu.make_async_remote_copy(
                src_ref=vbuf.at[piece],
                dst_ref=vbuf.at[piece],
                send_sem=d_send.at[d, e],
                recv_sem=d_recv.at[d, e],
                device_id={"fiber": fiber_of(e)},
                device_id_type=MESH,
            )
            copy.start()
            shared.append(copy)
    count_load.wait()
    for j in range(own_users):
        scaled = reg_weight * counts_ref[pl.ds(j, 1), :].astype(jnp.float32)
        across = jnp.broadcast_to(scaled, (block, block))
        damp_ref[pl.ds(j * block, block), :] = jnp.broadcast_to(
            jnp.transpose(across)[:, :1], (block, damp_ref.shape[1])
        )
    item_load.wait()
    rating_load.wait()
    for copy in rating_sends + shared:
        copy.wait_recv()

    def user_terms(stage, col, j):
        rows_of_user = pbuf[stage, col, pl.ds(pl.multiple_of(j * block, block), block), :]
        base = (col * own_users + j) * per_user

        items = jnp.concatenate([vbuf[item_ref[base + i]] for i in range(per_user)], axis=0)
        ratings = jnp.concatenate([rbuf[pos_ref[base + i]] for i in range(per_user)], axis=1)
        predicted = lax.dot_general(
            rows_of_user, items, (((1,), (1,)), ((), ())), preferred_element_type=jnp.float32
        )
        ratings = ratings.astype(jnp.float32)
        if stage == 0:
            weights = jnp.where(ratings != 0, ratings - predicted, 0.0)
        else:
            weights = jnp.where(ratings != 0, predicted, 0.0)
        return jnp.dot(weights.astype(jnp.bfloat16), items, preferred_element_type=jnp.float32)

    def reduced(stage):
        for d in [0] + order:
            if d:
                gather_copy(stage, d).wait_recv()
            col = col_of(d)

            def one(j, carry):
                part[stage, d, j] = user_terms(stage, col, j)
                return carry

            lax.fori_loop(0, own_users, one, 0)
            if d:
                for j in range(own_users):
                    bit = 1
                    while bit < (d & -d):
                        scatter_copy(stage, d | bit, j).wait_recv()
                        part[stage, d, j] = part[stage, d, j] + recv[stage, d | bit, j]
                        bit *= 2
                    scatter_copy(stage, d, j).start()
        totals = []
        for j in range(own_users):
            total = part[stage, 0, j]
            bit = 1
            while bit < cols:
                scatter_copy(stage, bit, j).wait_recv()
                total = total + recv[stage, bit, j]
                bit *= 2
            totals.append(total)
        return jnp.concatenate(totals, axis=0)

    residual = reduced(0) - damp_ref[...] * x_ref[...]
    r_ref[...] = residual
    p_ref[...] = residual
    squares = jnp.sum(residual * residual, axis=1, keepdims=True)
    for iteration in range(ITERS):
        pbuf[iteration + 1, my_col] = p_ref[...].astype(jnp.bfloat16)
        for d in order:
            gather_copy(iteration + 1, d).start()
        image = reduced(iteration + 1) + damp_ref[...] * p_ref[...]
        direction = p_ref[...]
        step_size = squares / (jnp.sum(direction * image, axis=1, keepdims=True) + tiny)
        x_ref[...] = x_ref[...] + step_size * direction
        residual = r_ref[...] - step_size * image
        r_ref[...] = residual
        if iteration + 1 < ITERS:
            renewed = jnp.sum(residual * residual, axis=1, keepdims=True)
            p_ref[...] = residual + renewed / (squares + tiny) * direction
            squares = renewed

    for copy in item_sends + rating_sends + shared:
        copy.wait_send()
    for stage in range(ITERS + 1):
        for d in range(1, cols):
            gather_copy(stage, d).wait_send()
            for j in range(own_users):
                scatter_copy(stage, d, j).wait_send()


def per_device(sizes, slab_users, user_factors, item_factors, ratings, block_user, block_item, counts):
    rows, cols, fibers = sizes
    held_blocks, block = ratings.shape[2], ratings.shape[3]
    rank = user_factors.shape[1]
    users = user_factors.shape[0]
    own_users = users // block
    item_blocks = item_factors.shape[0] // block
    per_user = fibers * held_blocks // (slab_users // block)

    both = lax.all_gather(jnp.stack([block_user[0, 0], block_item[0, 0]]), "fiber", axis=0)
    owners = both[:, 0].reshape(-1)
    columns = both[:, 1].reshape(-1)
    here = jnp.arange(owners.shape[0], dtype=jnp.int32)
    keys = owners * owners.shape[0] + here
    ranks = jnp.sum((keys[None, :] < keys[:, None]).astype(jnp.int32), axis=1)
    groups = jnp.arange(cols, dtype=jnp.int32)[:, None] * fibers + lax.axis_index("fiber")
    wanted = (
        groups[:, :, None] * (own_users * per_user)
        + jnp.arange(own_users * per_user, dtype=jnp.int32)[None, None, :]
    ).reshape(-1)
    match = wanted[:, None] == ranks[None, :]
    positions = jnp.sum(jnp.where(match, here[None, :], 0), axis=1)
    items = jnp.sum(jnp.where(match, columns[None, :], 0), axis=1)

    stages = ITERS + 1
    dma = pltpu.SemaphoreType.DMA
    vmem = pl.BlockSpec(memory_space=pltpu.VMEM)
    smem = pl.BlockSpec(memory_space=pltpu.SMEM)
    hbm = pl.BlockSpec(memory_space=pl.ANY)
    return pl.pallas_call(
        functools.partial(sweep_kernel, sizes),
        out_shape=(
            jax.ShapeDtypeStruct((users, rank), jnp.float32),
            jax.ShapeDtypeStruct((users, rank), jnp.float32),
        ),
        in_specs=[smem, smem, hbm, hbm, hbm, hbm],
        out_specs=(vmem, vmem),
        scratch_shapes=[
            pltpu.VMEM((rows * item_blocks, block, rank), jnp.bfloat16),
            pltpu.VMEM((fibers * held_blocks, block, block), jnp.bfloat16),
            pltpu.VMEM((stages, cols, users, rank), jnp.bfloat16),
            pltpu.VMEM((stages, cols, own_users, block, rank), jnp.float32),
            pltpu.VMEM((stages, cols, own_users, block, rank), jnp.float32),
            pltpu.VMEM((users, rank), jnp.float32),
            pltpu.VMEM((users, rank), jnp.float32),
            pltpu.VMEM((own_users, block), jnp.int32),
            dma,
            dma,
            dma,
            dma,
            dma((rows,)),
            dma((rows,)),
            dma((rows, fibers)),
            dma((rows, fibers)),
            dma((fibers,)),
            dma((fibers,)),
            dma((stages, cols)),
            dma((stages, cols)),
            dma((stages, cols, own_users)),
            dma((stages, cols, own_users)),
        ],
        compiler_params=pltpu.CompilerParams(
            collective_id=0, has_side_effects=True, vmem_limit_bytes=67043328
        ),
    )(
        positions,
        items,
        user_factors,
        counts.reshape(own_users, block),
        item_factors.reshape(item_blocks, block, rank),
        ratings[0, 0],
    )


def solution(mesh):
    sizes = (mesh.shape["row"], mesh.shape["col"], mesh.shape["fiber"])

    def whole(user_factors, item_factors, ratings, block_user, block_item, counts):
        slab_users = user_factors.shape[0] // sizes[0]
        return jax.shard_map(
            functools.partial(per_device, sizes, slab_users),
            mesh=mesh,
            in_specs=(
                P(("row", "col", "fiber"), None),
                P(("row", "col"), None),
                P("row", "col", "fiber", None, None),
                P("row", "col", "fiber"),
                P("row", "col", "fiber"),
                P(("row", "col", "fiber")),
            ),
            out_specs=(P(("row", "col", "fiber"), None), P(("row", "col", "fiber"), None)),
            check_vma=False,
        )(user_factors, item_factors, ratings, block_user, block_item, counts)

    return whole
```

```python
import functools

import jax
import jax.numpy as jnp
from jax import lax
from jax.experimental import pallas as pl
from jax.experimental.pallas import tpu as pltpu
from jax.sharding import PartitionSpec as P

ITERS = 2

reg_weight = 0.0004
tiny = 1e-06

MESH = pl.DeviceIdType.MESH


def sweep_kernel(
    sizes, pos_ref, item_ref, uf_hbm, counts_hbm, items_hbm, ratings_hbm, x_ref, r_ref,
    vbuf, rbuf, pbuf, part, recv, p_ref, damp_ref, counts_ref,
    user_sem, count_sem, item_sem, rating_sem, v_send, v_recv, d_send, d_recv, t_send, t_recv, g_send, g_recv, s_send, s_recv,
):
    rows, cols, fibers = sizes
    my_row, my_col, my_fiber = lax.axis_index("row"), lax.axis_index("col"), lax.axis_index("fiber")
    held_items = items_hbm.shape[0]
    share = held_items // fibers
    held_blocks, block = ratings_hbm.shape[0], ratings_hbm.shape[1]
    own_users = uf_hbm.shape[0] // block
    per_user = pos_ref.shape[0] // (cols * own_users)

    def row_of(d):
        return lax.rem(my_row + d, rows)

    def col_of(d):
        col, bit = my_col, 1
        while bit <= d:
            if d & bit:
                col = col + bit * (1 - 2 * lax.rem(lax.div(my_col, bit), 2))
            bit *= 2
        return col

    def fiber_of(d):
        return lax.rem(my_fiber + d, fibers)

    user_load = pltpu.make_async_copy(uf_hbm, x_ref, user_sem)
    user_load.start()
    count_load = pltpu.make_async_copy(counts_hbm, counts_ref, count_sem)
    count_load.start()
    own_items = pl.ds(my_row * held_items, held_items)
    item_load = pltpu.make_async_copy(items_hbm, vbuf.at[own_items], item_sem)
    item_load.start()
    own_ratings = pl.ds(my_fiber * held_blocks, held_blocks)
    rating_load = pltpu.make_async_copy(ratings_hbm, rbuf.at[own_ratings], rating_sem)
    rating_load.start()

    barrier = pltpu.get_barrier_semaphore()
    for d in range(1, rows):
        pl.semaphore_signal(barrier, inc=1, device_id={"row": row_of(d)}, device_id_type=MESH)
    for d in range(1, cols):
        pl.semaphore_signal(barrier, inc=1, device_id={"col": col_of(d)}, device_id_type=MESH)
    for d in range(1, fibers):
        pl.semaphore_signal(barrier, inc=1, device_id={"fiber": fiber_of(d)}, device_id_type=MESH)

    user_load.wait()
    for j in range(own_users):
        pbuf[0, my_col, j] = x_ref[pl.ds(j * block, block), :].astype(jnp.bfloat16)
    pl.semaphore_wait(barrier, rows + cols + fibers - 3)

    def gather_copy(stage, d, j):
        return pltpu.make_async_remote_copy(
            src_ref=pbuf.at[stage, my_col, j],
            dst_ref=pbuf.at[stage, my_col, j],
            send_sem=g_send.at[stage, d, j],
            recv_sem=g_recv.at[stage, d, j],
            device_id={"col": col_of(d)},
            device_id_type=MESH,
        )

    def scatter_copy(stage, d, j):
        return pltpu.make_async_remote_copy(
            src_ref=part.at[stage, d, j],
            dst_ref=recv.at[stage, d, j],
            send_sem=s_send.at[stage, d, j],
            recv_sem=s_recv.at[stage, d, j],
            device_id={"col": col_of(d & -d)},
            device_id_type=MESH,
        )

    item_sends = []
    for d in range(1, rows):
        copy = pltpu.make_async_remote_copy(
            src_ref=items_hbm.at[pl.ds(my_fiber * share, share)],
            dst_ref=vbuf.at[pl.ds(my_row * held_items + my_fiber * share, share)],
            send_sem=v_send.at[d],
            recv_sem=v_recv.at[d],
            device_id={"row": row_of(d)},
            device_id_type=MESH,
        )
        copy.start()
        item_sends.append(copy)
    order = sorted(range(1, cols), key=lambda d: (d & -d, -d))
    for j in range(own_users):
        for d in order:
            gather_copy(0, d, j).start()
    rating_sends = []
    for e in range(1, fibers):
        copy = pltpu.make_async_remote_copy(
            src_ref=ratings_hbm,
            dst_ref=rbuf.at[own_ratings],
            send_sem=t_send.at[e],
            recv_sem=t_recv.at[e],
            device_id={"fiber": fiber_of(e)},
            device_id_type=MESH,
        )
        copy.start()
        rating_sends.append(copy)
    shared = []
    for d in range(1, rows):
        item_sends[d - 1].wait_recv()
        source = lax.rem(my_row + rows - d, rows)
        piece = pl.ds(source * held_items + my_fiber * share, share)
        for e in range(1, fibers):
            copy = pltpu.make_async_remote_copy(
                src_ref=vbuf.at[piece],
                dst_ref=vbuf.at[piece],
                send_sem=d_send.at[d, e],
                recv_sem=d_recv.at[d, e],
                device_id={"fiber": fiber_of(e)},
                device_id_type=MESH,
            )
            copy.start()
            shared.append(copy)
    count_load.wait()
    for j in range(own_users):
        scaled = reg_weight * counts_ref[pl.ds(j, 1), :].astype(jnp.float32)
        across = jnp.broadcast_to(scaled, (block, block))
        damp_ref[pl.ds(j * block, block), :] = jnp.broadcast_to(
            jnp.transpose(across)[:, :1], (block, damp_ref.shape[1])
        )
    item_load.wait()
    rating_load.wait()
    for copy in rating_sends + shared:
        copy.wait_recv()

    def user_terms(stage, col, j):
        rows_of_user = pbuf[stage, col, j]
        base = (col * own_users + j) * per_user

        items = jnp.concatenate([vbuf[item_ref[base + i]] for i in range(per_user)], axis=0)
        ratings = jnp.concatenate([rbuf[pos_ref[base + i]] for i in range(per_user)], axis=1)
        predicted = lax.dot_general(
            rows_of_user, items, (((1,), (1,)), ((), ())), preferred_element_type=jnp.float32
        )
        ratings = ratings.astype(jnp.float32)
        if stage == 0:
            weights = jnp.where(ratings != 0, ratings - predicted, 0.0)
        else:
            weights = jnp.where(ratings != 0, predicted, 0.0)
        return jnp.dot(weights.astype(jnp.bfloat16), items, preferred_element_type=jnp.float32)

    def add_received(stage, d, j):
        total = part[stage, d, j]
        bit = 1
        while bit < (d & -d if d else cols):
            scatter_copy(stage, d | bit, j).wait_recv()
            total = total + recv[stage, d | bit, j]
            bit *= 2
        return total

    def scatter(stage):
        for j in range(own_users):
            for d in [0] + order:
                if d:
                    gather_copy(stage, d, j).wait_recv()
                part[stage, d, j] = user_terms(stage, col_of(d), j)
                if d & 1:
                    scatter_copy(stage, d, j).start()
        for d in order:
            if d & 1 == 0:
                for j in range(own_users):
                    part[stage, d, j] = add_received(stage, d, j)
                    scatter_copy(stage, d, j).start()

    def begin(stage, j, direction):
        users = pl.ds(j * block, block)
        p_ref[users, :] = direction
        pbuf[stage, my_col, j] = direction.astype(jnp.bfloat16)
        for d in order:
            gather_copy(stage, d, j).start()

    scatter(0)
    squares = []
    for j in range(own_users):
        users = pl.ds(j * block, block)
        residual = add_received(0, 0, j) - damp_ref[users, :] * x_ref[users, :]
        begin(1, j, residual)
        r_ref[users, :] = residual
        squares.append(jnp.sum(residual * residual, axis=1, keepdims=True))
    for iteration in range(ITERS):
        scatter(iteration + 1)
        for j in range(own_users):
            users = pl.ds(j * block, block)
            direction = p_ref[users, :]
            image = add_received(iteration + 1, 0, j) + damp_ref[users, :] * direction
            step_size = squares[j] / (jnp.sum(direction * image, axis=1, keepdims=True) + tiny)
            residual = r_ref[users, :] - step_size * image
            if iteration + 1 < ITERS:
                renewed = jnp.sum(residual * residual, axis=1, keepdims=True)
                begin(iteration + 2, j, residual + renewed / (squares[j] + tiny) * direction)
                squares[j] = renewed
            r_ref[users, :] = residual
            x_ref[users, :] = x_ref[users, :] + step_size * direction

    for copy in item_sends + rating_sends + shared:
        copy.wait_send()
    for stage in range(ITERS + 1):
        for d in range(1, cols):
            for j in range(own_users):
                gather_copy(stage, d, j).wait_send()
                scatter_copy(stage, d, j).wait_send()


def per_device(sizes, slab_users, user_factors, item_factors, ratings, block_user, block_item, counts):
    rows, cols, fibers = sizes
    held_blocks, block = ratings.shape[2], ratings.shape[3]
    rank = user_factors.shape[1]
    users = user_factors.shape[0]
    own_users = users // block
    item_blocks = item_factors.shape[0] // block
    per_user = fibers * held_blocks // (slab_users // block)

    both = lax.all_gather(jnp.stack([block_user[0, 0], block_item[0, 0]]), "fiber", axis=0)
    owners = both[:, 0].reshape(-1)
    columns = both[:, 1].reshape(-1)
    here = jnp.arange(owners.shape[0], dtype=jnp.int32)
    keys = owners * owners.shape[0] + here
    ranks = jnp.sum((keys[None, :] < keys[:, None]).astype(jnp.int32), axis=1)
    groups = jnp.arange(cols, dtype=jnp.int32)[:, None] * fibers + lax.axis_index("fiber")
    wanted = (
        groups[:, :, None] * (own_users * per_user)
        + jnp.arange(own_users * per_user, dtype=jnp.int32)[None, None, :]
    ).reshape(-1)
    match = wanted[:, None] == ranks[None, :]
    positions = jnp.sum(jnp.where(match, here[None, :], 0), axis=1)
    items = jnp.sum(jnp.where(match, columns[None, :], 0), axis=1)

    stages = ITERS + 1
    dma = pltpu.SemaphoreType.DMA
    vmem = pl.BlockSpec(memory_space=pltpu.VMEM)
    smem = pl.BlockSpec(memory_space=pltpu.SMEM)
    hbm = pl.BlockSpec(memory_space=pl.ANY)
    return pl.pallas_call(
        functools.partial(sweep_kernel, sizes),
        out_shape=(
            jax.ShapeDtypeStruct((users, rank), jnp.float32),
            jax.ShapeDtypeStruct((users, rank), jnp.float32),
        ),
        in_specs=[smem, smem, hbm, hbm, hbm, hbm],
        out_specs=(vmem, vmem),
        scratch_shapes=[
            pltpu.VMEM((rows * item_blocks, block, rank), jnp.bfloat16),
            pltpu.VMEM((fibers * held_blocks, block, block), jnp.bfloat16),
            pltpu.VMEM((stages, cols, own_users, block, rank), jnp.bfloat16),
            pltpu.VMEM((stages, cols, own_users, block, rank), jnp.float32),
            pltpu.VMEM((stages, cols, own_users, block, rank), jnp.float32),
            pltpu.VMEM((users, rank), jnp.float32),
            pltpu.VMEM((users, rank), jnp.float32),
            pltpu.VMEM((own_users, block), jnp.int32),
            dma,
            dma,
            dma,
            dma,
            dma((rows,)),
            dma((rows,)),
            dma((rows, fibers)),
            dma((rows, fibers)),
            dma((fibers,)),
            dma((fibers,)),
            dma((stages, cols, own_users)),
            dma((stages, cols, own_users)),
            dma((stages, cols, own_users)),
            dma((stages, cols, own_users)),
        ],
        compiler_params=pltpu.CompilerParams(
            collective_id=0, has_side_effects=True, vmem_limit_bytes=67043328
        ),
    )(
        positions,
        items,
        user_factors,
        counts.reshape(own_users, block),
        item_factors.reshape(item_blocks, block, rank),
        ratings[0, 0],
    )


def solution(mesh):
    sizes = (mesh.shape["row"], mesh.shape["col"], mesh.shape["fiber"])

    def whole(user_factors, item_factors, ratings, block_user, block_item, counts):
        slab_users = user_factors.shape[0] // sizes[0]
        return jax.shard_map(
            functools.partial(per_device, sizes, slab_users),
            mesh=mesh,
            in_specs=(
                P(("row", "col", "fiber"), None),
                P(("row", "col"), None),
                P("row", "col", "fiber", None, None),
                P("row", "col", "fiber"),
                P("row", "col", "fiber"),
                P(("row", "col", "fiber")),
            ),
            out_specs=(P(("row", "col", "fiber"), None), P(("row", "col", "fiber"), None)),
            check_vma=False,
        )(user_factors, item_factors, ratings, block_user, block_item, counts)

    return whole
```
